32 devices in a mesh: dp: 4 (over y, core), tensor: 8 (over z, x).
Axes of the slice: x: 2, y: 2, z: 4, core: 2. Of those that a mesh axis runs over, the one named last changes fastest.
Arguments:
- attn_input: bfloat16 [512, 8192], P('dp'), may hold values from -6 to 6
- residual: bfloat16 [512, 8192], P('dp'), may hold values from -3 to 3
- query_weight: bfloat16 [8192, 2048], P('dp', 'tensor'), may hold values from -0.0625 to 0.0625
- query_bias: bfloat16 [2048], P('tensor'), may hold values from -3 to 3
- output_weight: bfloat16 [2048, 8192], P('tensor', 'dp'), may hold values from -0.125 to 0.125
- cached_keys: bfloat16 [4, 8, 1024, 128], P('dp', 'tensor'), may hold values from -305 to 305, as said below
- cached_values: bfloat16 [4, 8, 1024, 128], P('dp', 'tensor'), may hold values from -12 to 12, as said below
- norm_gain: bfloat16 [8192], replicated, may hold values from 0.5 to 1.5
Outputs:
- hidden_out: bfloat16 [512, 8192], P(('dp', 'tensor'))
- normed_out: bfloat16 [512, 8192], P('dp')
The draws below stay inside these ranges and needn't reach their ends.
Inputs may be any that keep to these rules, and one draw needn't show every extreme that they name: `cached_keys`: groups g and g2 with g // 1 == g2 // 1 carry equal keys. `cached_values`: groups g and g2 with g // 1 == g2 // 1 carry equal values.
All inputs are finite; a program needn't handle non-finite values.
Results may differ from the reference program's by a relative error of at most 0.025.
Values may be sent and summed in bfloat16 or wider, within the bound.
No kernel may reach another device: no remote copies, remote signals or barrier semaphores. Data moves between devices by JAX's collectives and lax.ppermute only.
A program may use at most 64 MiB of HBM per device.

```python
import jax
import jax.numpy as jnp
from jax import lax

D = 8192
HD = 128
KVH = 8
QH_DEV = 2
TOK = 128
CTX = 1024
HEADS = 16
N_DP = 4
N_TENSOR = 8


def draw_cached_keys(key, part):
    base_key = jax.random.fold_in(key, 11)
    full_shape = (N_DP, KVH, CTX, HD)
    drawn = 2.0 * jax.random.truncated_normal(base_key, -6.0, 6.0, full_shape, jnp.float32)
    packed = drawn.astype(jnp.bfloat16)
    return jnp.repeat(packed, N_TENSOR // KVH, axis=1)


def draw_cached_values(key, part):
    base_key = jax.random.fold_in(key, 37)
    full_shape = (N_DP, KVH, CTX, HD)
    drawn = 2.0 * jax.random.truncated_normal(base_key, -6.0, 6.0, full_shape, jnp.float32)
    packed = drawn.astype(jnp.bfloat16)
    return jnp.repeat(packed, N_TENSOR // KVH, axis=1)


def levels(key, shape, cuts, least, largest):
    loudness, own = 1.0, jax.random.fold_in(key, 6)
    for dim, shards_of in cuts:
        steps = jnp.exp(jax.random.uniform(jax.random.fold_in(own, dim), (shards_of,), jnp.float32, least / len(cuts), largest / len(cuts)))
        loudness = loudness * jnp.repeat(steps, shape[dim] // shards_of).reshape([-1 if axis == dim else 1 for axis in range(len(shape))])
    return loudness


def noise(rng, shape, scale, limit, pieces=(), kind=jnp.bfloat16):
    values = jax.random.normal(rng, shape, jnp.float32) * scale
    if len(pieces) > 0:
        values = levels(rng, shape, pieces, -0.22, 0.18) * values
    return jnp.clip(values, min=-limit, max=limit).astype(kind)


def setup_inputs(seed: int = 0) -> dict:
    arg_keys = jax.random.split(jax.random.key(seed), 9)
    return {
        "attn_input": noise(arg_keys[0], (N_DP * TOK, D), 1.0, 6.0, ((0, 4),)),
        "residual": noise(arg_keys[1], (N_DP * TOK, D), 0.5, 3.0, ((0, 4),)),
        "query_weight": noise(arg_keys[2], (D, HEADS * HD), D ** -0.5, 0.0625, ((0, 4), (1, 8))),
        "query_bias": noise(arg_keys[3], (HEADS * HD,), 0.5, 3.0, ((0, 8),)),
        "output_weight": noise(arg_keys[4], (HEADS * HD, D), (HEADS * HD) ** -0.5, 0.125, ((0, 8), (1, 4))),
        "cached_keys": draw_cached_keys(jax.random.fold_in(arg_keys[8], 71), 0),
        "cached_values": draw_cached_values(jax.random.fold_in(arg_keys[8], 71), 0),
        "norm_gain": jnp.clip(1.0 + 0.1 * jax.random.normal(arg_keys[7], (D,), jnp.float32), 0.5, 1.5).astype(jnp.bfloat16),
    }


rope_theta = 1000000.0
norm_eps = 1e-06

def rotate(projected, first_pos):
    head_dim = projected.shape[-1]
    half_dim = head_dim // 2
    inv_freq = jnp.power(jnp.float32(rope_theta), -2.0 * jnp.arange(half_dim, dtype=jnp.float32) / head_dim)
    positions = first_pos + jnp.arange(projected.shape[0], dtype=jnp.float32)
    angles = positions[:, None] * inv_freq[None, :]
    cosine = jnp.cos(angles)[:, None, :]
    sine = jnp.sin(angles)[:, None, :]
    first_half = projected[..., :half_dim]
    second_half = projected[..., half_dim:]
    return jnp.concatenate([first_half * cosine - second_half * sine, second_half * cosine + first_half * sine], axis=-1)

def attend(queries, group_keys, group_values):
    count_q = queries.shape[0]
    groups = group_keys.shape[0]
    count_k = group_keys.shape[1]
    grouped = queries.reshape(count_q, groups, queries.shape[1] // groups, queries.shape[2]).astype(jnp.float32)
    scores = jnp.einsum('tgqd,gkd->gqtk', grouped, group_keys.astype(jnp.float32)) * (1.0 / queries.shape[-1] ** 0.5)
    visible = jnp.arange(count_k)[None, :] <= (count_k - count_q + jnp.arange(count_q))[:, None]
    scores = jnp.where(visible[None, None], scores, jnp.float32(-1e+30))
    highest = lax.optimization_barrier(jnp.max(scores, axis=-1, keepdims=True))
    expo = jnp.exp(scores - highest)
    soft = (expo / lax.optimization_barrier(jnp.sum(expo, axis=-1, keepdims=True))).astype(jnp.bfloat16)
    mixed = jnp.einsum('gqtk,gkd->tgqd', soft.astype(jnp.float32), group_values.astype(jnp.float32))
    return mixed.reshape(queries.shape).astype(jnp.bfloat16)

def reference(attn_input, residual, query_weight, query_bias, output_weight, cached_keys, cached_values, norm_gain):
    groups = HEADS // QH_DEV
    weight_blocks = output_weight.reshape(groups, QH_DEV * HD, D)

    def one_sequence(group_items):
        inputs, resid_rows, group_keys, group_values = group_items
        projected = jnp.dot(inputs, query_weight, preferred_element_type=jnp.float32) + query_bias.astype(jnp.float32)
        queries = rotate(projected.reshape(TOK, HEADS, HD), float(CTX - TOK)).astype(jnp.bfloat16)
        mixed = attend(queries, group_keys, group_values).reshape(TOK, groups, QH_DEV * HD).transpose(1, 0, 2)

        def add_group(running, operands):
            group_part = jnp.dot(operands[0], operands[1], preferred_element_type=jnp.float32).astype(jnp.bfloat16)
            group_part = lax.optimization_barrier(group_part)
            return (running + group_part.astype(jnp.float32), None)
        summed, unused = lax.scan(add_group, jnp.zeros((TOK, D), jnp.float32), (mixed, weight_blocks))
        total = resid_rows.astype(jnp.float32) + summed
        mean_square = lax.optimization_barrier(jnp.mean(total * total, axis=-1, keepdims=True))
        normed = total * lax.rsqrt(mean_square + norm_eps) * norm_gain.astype(jnp.float32)
        return (total.astype(jnp.bfloat16), normed.astype(jnp.bfloat16))
    hidden, normed = lax.map(one_sequence, (attn_input.reshape(N_DP, TOK, D), residual.reshape(N_DP, TOK, D), cached_keys, cached_values))
    return (hidden.reshape(N_DP * TOK, D), normed.reshape(N_DP * TOK, D))
```

```python
import jax
import jax.numpy as jnp
from jax import lax
from jax.experimental import pallas as pl
from jax.experimental.pallas import tpu as pltpu
from jax.sharding import PartitionSpec as P

rope_theta = 1000000.0
norm_eps = 1e-06


def rotate(projected, first_pos):
    head_dim = projected.shape[-1]
    half_dim = head_dim // 2
    inv_freq = jnp.power(
        jnp.float32(rope_theta), -2.0 * jnp.arange(half_dim, dtype=jnp.float32) / head_dim
    )
    positions = first_pos + jnp.arange(projected.shape[0], dtype=jnp.float32)
    angles = positions[:, None] * inv_freq[None, :]
    cosine = jnp.cos(angles)[:, None, :]
    sine = jnp.sin(angles)[:, None, :]
    first_half = projected[..., :half_dim]
    second_half = projected[..., half_dim:]
    return jnp.concatenate(
        [first_half * cosine - second_half * sine, second_half * cosine + first_half * sine],
        axis=-1,
    )


def attend(queries, local_keys, local_values):
    count_q = queries.shape[0]
    count_k = local_keys.shape[0]
    scores = jnp.einsum("thd,kd->htk", queries, local_keys, preferred_element_type=jnp.float32) * (
        1.0 / queries.shape[-1] ** 0.5
    )
    visible = jnp.arange(count_k)[None, :] <= (count_k - count_q + jnp.arange(count_q))[:, None]
    scores = jnp.where(visible[None], scores, jnp.float32(-1e30))
    highest = jnp.max(scores, axis=-1, keepdims=True)
    expo = jnp.exp(scores - highest)
    soft = (expo / jnp.sum(expo, axis=-1, keepdims=True)).astype(jnp.bfloat16)
    mixed = jnp.einsum("htk,kd->thd", soft, local_values, preferred_element_type=jnp.float32)
    return mixed.astype(jnp.bfloat16)


def normalize(total, norm_gain):
    mean_square = jnp.mean(total * total, axis=-1, keepdims=True)
    return (total * lax.rsqrt(mean_square + norm_eps) * norm_gain.astype(jnp.float32)).astype(
        jnp.bfloat16
    )


def gathered_body(
    attn_input,
    residual,
    query_weight,
    query_bias,
    output_weight,
    cached_keys,
    cached_values,
    norm_gain,
):
    tok_count = attn_input.shape[0]
    ctx_len = cached_keys.shape[2]
    head_dim = cached_keys.shape[3]
    local_heads = query_weight.shape[1] // head_dim
    projected = jnp.dot(
        attn_input,
        lax.all_gather(query_weight, "dp", axis=0, tiled=True),
        preferred_element_type=jnp.float32,
    )
    projected = projected + query_bias.astype(jnp.float32)
    queries = rotate(
        projected.reshape(tok_count, local_heads, head_dim), float(ctx_len - tok_count)
    ).astype(jnp.bfloat16)
    mixed = attend(queries, cached_keys[0, 0], cached_values[0, 0]).reshape(
        tok_count, local_heads * head_dim
    )
    partial_sum = jnp.dot(
        mixed,
        lax.all_gather(output_weight, "dp", axis=1, tiled=True),
        preferred_element_type=jnp.float32,
    )
    own_count = tok_count // lax.axis_size("tensor")
    own_start = lax.axis_index("tensor") * own_count
    summed = lax.psum(partial_sum.astype(jnp.bfloat16), "tensor").astype(jnp.float32)
    total = residual.astype(jnp.float32) + summed
    normed_out = normalize(total, norm_gain)
    hidden_out = lax.dynamic_slice_in_dim(total, own_start, own_count, 0).astype(jnp.bfloat16)
    return (hidden_out, normed_out)


def ring_order(count):
    return list(range(0, count, 2)) + list(range(count - 1, 0, -2))


def shift_in_ring(value, step):
    count = lax.axis_size("tensor")
    order = ring_order(count)
    pairs = [(order[i], order[(i + step) % count]) for i in range(count)]
    return lax.ppermute(value, "tensor", pairs)


def ring_sources():
    count = lax.axis_size("tensor")
    order = ring_order(count)
    place = {device: i for i, device in enumerate(order)}
    table = [[order[(place[d] - k) % count] for k in range(count)] for d in range(count)]
    return jnp.array(table, jnp.int32)[lax.axis_index("tensor")]


def ring_gather(pieces):
    count = lax.axis_size("tensor")
    ahead, back = pieces, pieces
    found = {0: pieces}
    for k in range(1, count // 2 + 1):
        if 2 * k < count:
            ahead = [shift_in_ring(piece, 1) for piece in ahead]
            back = [shift_in_ring(piece, -1) for piece in back]
            found[k], found[count - k] = ahead, back
        else:
            half = (len(pieces) + 1) // 2
            found[k] = [shift_in_ring(piece, 1) for piece in ahead[:half]] + [
                shift_in_ring(piece, -1) for piece in back[half:]
            ]
    return [found[k] for k in range(count)]


def swap_pair(value):
    count = lax.axis_size("dp")
    return lax.ppermute(value, "dp", [(i, i ^ 1) for i in range(count)])


def shift_pairs(value):
    count = lax.axis_size("dp")
    return lax.ppermute(value, "dp", [(i, (i + 2) % count) for i in range(count)])


def pair_gather(value, splits):
    count = lax.axis_size("dp")
    own = lax.axis_index("dp")
    rows = value.shape[0] // splits
    pieces = [value[i * rows : (i + 1) * rows] for i in range(splits)]
    found = []
    for k in range(count // 2):
        if k:
            pieces = [shift_pairs(piece) for piece in pieces]
        found.append(((own - 2 * k) % count, pieces))
        found.append((((own ^ 1) - 2 * k) % count, [swap_pair(piece) for piece in pieces]))
    return found


def finish_kernel(offsets, first_row, gain, *refs, width):
    chunks, (hidden, normed) = refs[:-2], refs[-2:]
    features = normed.shape[1]
    blocks = chunks[0].shape[1] // width
    squares = jnp.zeros((normed.shape[0], 128), jnp.float32)
    for chunk in chunks:
        for i in range(chunk.shape[1] // 128):
            part = chunk[:, i * 128 : (i + 1) * 128].astype(jnp.float32)
            squares = squares + part * part
    scale = lax.rsqrt(jnp.sum(squares, axis=1, keepdims=True) / features + norm_eps)
    own_rows = pl.ds(pl.multiple_of(first_row[0], hidden.shape[0]), hidden.shape[0])
    for k, chunk in enumerate(chunks):
        for i in range(blocks):
            columns = pl.ds(pl.multiple_of(offsets[k * blocks + i], 128), width)
            part = chunk[:, i * width : (i + 1) * width].astype(jnp.float32)
            normed[:, columns] = (part * scale * gain[:, columns].astype(jnp.float32)).astype(
                jnp.bfloat16
            )
            hidden[:, columns] = chunk[own_rows, i * width : (i + 1) * width]


def finish(chunks, offsets, first_row, own_count, norm_gain, width):
    rows = chunks[0].shape[0]
    features = norm_gain.shape[0]
    smem = pl.BlockSpec(memory_space=pltpu.SMEM)
    vmem = pl.BlockSpec(memory_space=pltpu.VMEM)
    return pl.pallas_call(
        lambda *refs: finish_kernel(*refs, width=width),
        out_shape=(
            jax.ShapeDtypeStruct((own_count, features), jnp.bfloat16),
            jax.ShapeDtypeStruct((rows, features), jnp.bfloat16),
        ),
        in_specs=[smem, smem] + [vmem] * (1 + len(chunks)),
        out_specs=(vmem, vmem),
        name="finish",
    )(offsets, first_row.reshape(1), norm_gain.reshape(1, features), *chunks)


def exchanged_body(
    attn_input,
    residual,
    query_weight,
    query_bias,
    output_weight,
    cached_keys,
    cached_values,
    norm_gain,
):
    tok_count = attn_input.shape[0]
    ctx_len = cached_keys.shape[2]
    head_dim = cached_keys.shape[3]
    local_heads = query_weight.shape[1] // head_dim
    count_t = lax.axis_size("tensor")
    own_t = lax.axis_index("tensor")
    own_rows = query_weight.shape[0]
    shard_cols = output_weight.shape[1]
    width = shard_cols // count_t
    sources = ring_sources()
    forward = [sources[(count_t - k) % count_t] for k in range(count_t)]

    heads_of = [
        lax.dynamic_slice_in_dim(output_weight, forward[k] * width, width, 1)
        for k in range(count_t)
    ]
    heads_of = [shift_in_ring(block, k) if k else block for k, block in enumerate(heads_of)]

    splits = 2
    projected = query_bias.astype(jnp.float32)
    for owner, pieces in pair_gather(query_weight, splits):
        rows = own_rows // splits
        for i, piece in enumerate(pieces):
            part = lax.dynamic_slice_in_dim(attn_input, owner * own_rows + i * rows, rows, 1)
            projected = projected + jnp.dot(part, piece, preferred_element_type=jnp.float32)
    queries = rotate(
        projected.reshape(tok_count, local_heads, head_dim), float(ctx_len - tok_count)
    ).astype(jnp.bfloat16)
    mixed = attend(queries, cached_keys[0, 0], cached_values[0, 0]).reshape(
        tok_count, local_heads * head_dim
    )
    mixed = jnp.concatenate([got[0] for got in ring_gather([mixed])], axis=1)

    column_weight = jnp.concatenate(heads_of, axis=0)
    blocks, owners = [], []
    for owner, pieces in pair_gather(column_weight, splits):
        rows = column_weight.shape[0] // splits
        summed = sum(
            jnp.dot(
                mixed[:, i * rows : (i + 1) * rows], piece, preferred_element_type=jnp.float32
            )
            for i, piece in enumerate(pieces)
        )
        start = owner * shard_cols + own_t * width
        resid = lax.dynamic_slice_in_dim(residual, start, width, 1).astype(jnp.float32)
        blocks.append((resid + summed).astype(jnp.bfloat16))
        owners.append(owner)
    total = jnp.concatenate(blocks, axis=1)

    own_count = tok_count // count_t
    chunks = [got[0] for got in ring_gather([total])]
    offsets = (sources[:, None] * width + jnp.stack(owners)[None, :] * shard_cols).reshape(-1)
    return finish(chunks, offsets.astype(jnp.int32), own_t * own_count, own_count, norm_gain, width)


def body(*arrays):
    output_weight = arrays[4]
    width = output_weight.shape[1] // lax.axis_size("tensor")
    if width % 128 or lax.axis_size("tensor") % 2 or lax.axis_size("dp") % 2:
        return gathered_body(*arrays)
    return exchanged_body(*arrays)


def solution(mesh):
    return jax.shard_map(
        body,
        mesh=mesh,
        in_specs=(
            P("dp", None),
            P("dp", None),
            P("dp", "tensor"),
            P("tensor"),
            P("tensor", "dp"),
            P("dp", "tensor", None, None),
            P("dp", "tensor", None, None),
            P(),
        ),
        out_specs=(P(("dp", "tensor"), None), P("dp", None)),
        check_vma=False,
    )
```

```python
import jax
import jax.numpy as jnp
from jax import lax
from jax.experimental import pallas as pl
from jax.experimental.pallas import tpu as pltpu
from jax.sharding import PartitionSpec as P


rope_theta = 1000000.0
norm_eps = 1e-06


def rotate(projected, first_pos):
    head_dim = projected.shape[-1]
    half_dim = head_dim // 2
    inv_freq = jnp.power(
        jnp.float32(rope_theta), -2.0 * jnp.arange(half_dim, dtype=jnp.float32) / head_dim
    )
    positions = first_pos + jnp.arange(projected.shape[0], dtype=jnp.float32)
    angles = positions[:, None] * inv_freq[None, :]
    cosine = jnp.cos(angles)[:, None, :]
    sine = jnp.sin(angles)[:, None, :]
    first_half = projected[..., :half_dim]
    second_half = projected[..., half_dim:]
    return jnp.concatenate(
        [first_half * cosine - second_half * sine, second_half * cosine + first_half * sine],
        axis=-1,
    )


def attend(queries, local_keys, local_values):
    count_q = queries.shape[0]
    count_k = local_keys.shape[0]
    scores = jnp.einsum("thd,kd->htk", queries, local_keys, preferred_element_type=jnp.float32) * (
        1.0 / queries.shape[-1] ** 0.5
    )
    visible = jnp.arange(count_k)[None, :] <= (count_k - count_q + jnp.arange(count_q))[:, None]
    scores = jnp.where(visible[None], scores, jnp.float32(-1e30))
    highest = jnp.max(scores, axis=-1, keepdims=True)
    expo = jnp.exp(scores - highest)
    soft = (expo / jnp.sum(expo, axis=-1, keepdims=True)).astype(jnp.bfloat16)
    mixed = jnp.einsum("htk,kd->thd", soft, local_values, preferred_element_type=jnp.float32)
    return mixed.astype(jnp.bfloat16)


def normalize(total, norm_gain):
    mean_square = jnp.mean(total * total, axis=-1, keepdims=True)
    return (total * lax.rsqrt(mean_square + norm_eps) * norm_gain.astype(jnp.float32)).astype(
        jnp.bfloat16
    )


def gathered_body(
    attn_input,
    residual,
    query_weight,
    query_bias,
    output_weight,
    cached_keys,
    cached_values,
    norm_gain,
):
    tok_count = attn_input.shape[0]
    ctx_len = cached_keys.shape[2]
    head_dim = cached_keys.shape[3]
    local_heads = query_weight.shape[1] // head_dim
    projected = jnp.dot(
        attn_input,
        lax.all_gather(query_weight, "dp", axis=0, tiled=True),
        preferred_element_type=jnp.float32,
    )
    projected = projected + query_bias.astype(jnp.float32)
    queries = rotate(
        projected.reshape(tok_count, local_heads, head_dim), float(ctx_len - tok_count)
    ).astype(jnp.bfloat16)
    mixed = attend(queries, cached_keys[0, 0], cached_values[0, 0]).reshape(
        tok_count, local_heads * head_dim
    )
    partial_sum = jnp.dot(
        mixed,
        lax.all_gather(output_weight, "dp", axis=1, tiled=True),
        preferred_element_type=jnp.float32,
    )
    own_count = tok_count // lax.axis_size("tensor")
    own_start = lax.axis_index("tensor") * own_count
    summed = lax.psum(partial_sum.astype(jnp.bfloat16), "tensor").astype(jnp.float32)
    total = residual.astype(jnp.float32) + summed
    normed_out = normalize(total, norm_gain)
    hidden_out = lax.dynamic_slice_in_dim(total, own_start, own_count, 0).astype(jnp.bfloat16)
    return (hidden_out, normed_out)


def ring_order(count):
    return list(range(0, count, 2)) + list(range(count - 1, 0, -2))


def shift_in_ring(value, step):
    count = lax.axis_size("tensor")
    order = ring_order(count)
    pairs = [(order[i], order[(i + step) % count]) for i in range(count)]
    return lax.ppermute(value, "tensor", pairs)


def ring_sources(own, count):
    place = jnp.where(own % 2 == 0, own // 2, count - 1 - own // 2)
    back = [(place - k) % count for k in range(count)]
    return [jnp.where(2 * p < count, 2 * p, 2 * (count - 1 - p) + 1) for p in back]


def ring_gather(value, last_step):
    count = lax.axis_size("tensor")
    ahead, back = value, value
    found = {0: value}
    for k in range(1, (count + 1) // 2):
        ahead = shift_in_ring(ahead, 1)
        back = shift_in_ring(back, -1)
        found[k], found[count - k] = ahead, back
    found[count // 2] = shift_in_ring(ahead if last_step > 0 else back, last_step)
    return [found[k] for k in range(count)]


def pair_owners(own, count):
    return [((own ^ (k % 2)) - 2 * (k // 2)) % count for k in range(count)]


def swap_pair(value):
    count = lax.axis_size("dp")
    return lax.ppermute(value, "dp", [(i, i ^ 1) for i in range(count)])


def shift_pairs(value):
    count = lax.axis_size("dp")
    return lax.ppermute(value, "dp", [(i, (i + 2) % count) for i in range(count)])


def pair_gather(value):
    count = lax.axis_size("dp")
    own = lax.axis_index("dp")
    found = []
    for k in range(count // 2):
        if k:
            value = shift_pairs(value)
        found.append(((own - 2 * k) % count, value))
        found.append((((own ^ 1) - 2 * k) % count, swap_pair(value)))
    return found


def finish_kernel(own_t, own_d, gain, *refs, width):
    chunks, (hidden, normed) = refs[:-2], refs[-2:]
    features = normed.shape[1]
    squares = jnp.zeros((normed.shape[0], 128), jnp.float32)
    for chunk in chunks:
        for i in range(chunk.shape[1] // 128):
            part = chunk[:, i * 128 : (i + 1) * 128].astype(jnp.float32)
            squares = squares + part * part
    scale = lax.rsqrt(jnp.sum(squares, axis=1, keepdims=True) / features + norm_eps)
    own_rows = pl.ds(pl.multiple_of(own_t[0] * hidden.shape[0], hidden.shape[0]), hidden.shape[0])
    per_chunk = chunks[0].shape[1] // width
    count_t = len(chunks) // 2
    sources = ring_sources(own_t[0], count_t)
    owners = pair_owners(own_d[0], 2 * per_chunk)
    for k, chunk in enumerate(chunks):
        for i in range(per_chunk):
            owner = owners[k % 2 * per_chunk + i]
            start = (owner * count_t + sources[k // 2]) * width
            columns = pl.ds(pl.multiple_of(start, 128), width)
            part = chunk[:, i * width : (i + 1) * width].astype(jnp.float32)
            normed[:, columns] = (part * scale * gain[:, columns].astype(jnp.float32)).astype(
                jnp.bfloat16
            )
            hidden[:, columns] = chunk[own_rows, i * width : (i + 1) * width]


def finish(chunks, own_count, norm_gain, width):
    rows = chunks[0].shape[0]
    features = norm_gain.shape[0]
    smem = pl.BlockSpec(memory_space=pltpu.SMEM)
    vmem = pl.BlockSpec(memory_space=pltpu.VMEM)
    return pl.pallas_call(
        lambda *refs: finish_kernel(*refs, width=width),
        out_shape=(
            jax.ShapeDtypeStruct((own_count, features), jnp.bfloat16),
            jax.ShapeDtypeStruct((rows, features), jnp.bfloat16),
        ),
        in_specs=[smem, smem] + [vmem] * (1 + len(chunks)),
        out_specs=(vmem, vmem),
        name="finish",
    )(
        lax.axis_index("tensor").reshape(1),
        lax.axis_index("dp").reshape(1),
        norm_gain.reshape(1, features),
        *chunks,
    )


def exchanged_body(
    attn_input,
    residual,
    query_weight,
    query_bias,
    output_weight,
    cached_keys,
    cached_values,
    norm_gain,
):
    tok_count = attn_input.shape[0]
    ctx_len = cached_keys.shape[2]
    head_dim = cached_keys.shape[3]
    local_heads = query_weight.shape[1] // head_dim
    count_t = lax.axis_size("tensor")
    own_t = lax.axis_index("tensor")
    own_rows = query_weight.shape[0]
    shard_cols = output_weight.shape[1]
    width = shard_cols // count_t

    column_weight = lax.all_to_all(output_weight, "tensor", 1, 0, tiled=True)

    projected = query_bias.astype(jnp.float32)
    for owner, shard in pair_gather(query_weight):
        part = lax.dynamic_slice_in_dim(attn_input, owner * own_rows, own_rows, 1)
        projected = projected + jnp.dot(part, shard, preferred_element_type=jnp.float32)
    queries = rotate(
        projected.reshape(tok_count, local_heads, head_dim), float(ctx_len - tok_count)
    ).astype(jnp.bfloat16)
    mixed = attend(queries, cached_keys[0, 0], cached_values[0, 0]).reshape(
        tok_count, local_heads * head_dim
    )
    head_cols = mixed.shape[1]
    gathered = jnp.zeros((tok_count, count_t * head_cols), jnp.bfloat16)
    for source, got in zip(ring_sources(own_t, count_t), ring_gather(mixed, 1)):
        gathered = lax.dynamic_update_slice_in_dim(gathered, got, source * head_cols, 1)

    blocks = []
    for owner, shard in pair_gather(column_weight):
        summed = jnp.dot(gathered, shard, preferred_element_type=jnp.float32)
        start = owner * shard_cols + own_t * width
        resid = lax.dynamic_slice_in_dim(residual, start, width, 1).astype(jnp.float32)
        blocks.append((resid + summed).astype(jnp.bfloat16))
    count = len(blocks) // 2
    parts = [jnp.concatenate(blocks[i * count : (i + 1) * count], axis=1) for i in range(2)]
    near = ring_gather(parts[0], 1)
    far = ring_gather(parts[1], -1)
    chunks = [chunk for got in zip(near, far) for chunk in got]
    return finish(chunks, tok_count // count_t, norm_gain, width)


def body(*arrays):
    output_weight = arrays[4]
    width = output_weight.shape[1] // lax.axis_size("tensor")
    if width % 128 or lax.axis_size("tensor") % 2 or lax.axis_size("dp") % 2:
        return gathered_body(*arrays)
    return exchanged_body(*arrays)


def solution(mesh):
    return jax.shard_map(
        body,
        mesh=mesh,
        in_specs=(
            P("dp", None),
            P("dp", None),
            P("dp", "tensor"),
            P("tensor"),
            P("tensor", "dp"),
            P("dp", "tensor", None, None),
            P("dp", "tensor", None, None),
            P(),
        ),
        out_specs=(P(("dp", "tensor"), None), P("dp", None)),
        check_vma=False,
    )
```

```python
import jax
import jax.numpy as jnp
from jax import lax
from jax.experimental import pallas as pl
from jax.experimental.pallas import tpu as pltpu
from jax.sharding import PartitionSpec as P


rope_theta = 1000000.0
norm_eps = 1e-06


def rotate(projected, first_pos):
    head_dim = projected.shape[-1]
    half_dim = head_dim // 2
    inv_freq = jnp.power(
        jnp.float32(rope_theta), -2.0 * jnp.arange(half_dim, dtype=jnp.float32) / head_dim
    )
    positions = first_pos + jnp.arange(projected.shape[0], dtype=jnp.float32)
    angles = positions[:, None] * inv_freq[None, :]
    cosine = jnp.cos(angles)[:, None, :]
    sine = jnp.sin(angles)[:, None, :]
    first_half = projected[..., :half_dim]
    second_half = projected[..., half_dim:]
    return jnp.concatenate(
        [first_half * cosine - second_half * sine, second_half * cosine + first_half * sine],
        axis=-1,
    )


def attend(queries, local_keys, local_values):
    count_q = queries.shape[0]
    count_k = local_keys.shape[0]
    scores = jnp.einsum("thd,kd->htk", queries, local_keys, preferred_element_type=jnp.float32) * (
        1.0 / queries.shape[-1] ** 0.5
    )
    visible = jnp.arange(count_k)[None, :] <= (count_k - count_q + jnp.arange(count_q))[:, None]
    scores = jnp.where(visible[None], scores, jnp.float32(-1e30))
    highest = jnp.max(scores, axis=-1, keepdims=True)
    expo = jnp.exp(scores - highest)
    soft = (expo / jnp.sum(expo, axis=-1, keepdims=True)).astype(jnp.bfloat16)
    mixed = jnp.einsum("htk,kd->thd", soft, local_values, preferred_element_type=jnp.float32)
    return mixed.astype(jnp.bfloat16)


def normalize(total, norm_gain):
    mean_square = jnp.mean(total * total, axis=-1, keepdims=True)
    return (total * lax.rsqrt(mean_square + norm_eps) * norm_gain.astype(jnp.float32)).astype(
        jnp.bfloat16
    )


def gathered_body(
    attn_input,
    residual,
    query_weight,
    query_bias,
    output_weight,
    cached_keys,
    cached_values,
    norm_gain,
):
    tok_count = attn_input.shape[0]
    ctx_len = cached_keys.shape[2]
    head_dim = cached_keys.shape[3]
    local_heads = query_weight.shape[1] // head_dim
    projected = jnp.dot(
        attn_input,
        lax.all_gather(query_weight, "dp", axis=0, tiled=True),
        preferred_element_type=jnp.float32,
    )
    projected = projected + query_bias.astype(jnp.float32)
    queries = rotate(
        projected.reshape(tok_count, local_heads, head_dim), float(ctx_len - tok_count)
    ).astype(jnp.bfloat16)
    mixed = attend(queries, cached_keys[0, 0], cached_values[0, 0]).reshape(
        tok_count, local_heads * head_dim
    )
    partial_sum = jnp.dot(
        mixed,
        lax.all_gather(output_weight, "dp", axis=1, tiled=True),
        preferred_element_type=jnp.float32,
    )
    own_count = tok_count // lax.axis_size("tensor")
    own_start = lax.axis_index("tensor") * own_count
    summed = lax.psum(partial_sum.astype(jnp.bfloat16), "tensor").astype(jnp.float32)
    total = residual.astype(jnp.float32) + summed
    normed_out = normalize(total, norm_gain)
    hidden_out = lax.dynamic_slice_in_dim(total, own_start, own_count, 0).astype(jnp.bfloat16)
    return (hidden_out, normed_out)


def ring_order(count):
    return list(range(0, count, 2)) + list(range(count - 1, 0, -2))


def shift_in_ring(value, step):
    count = lax.axis_size("tensor")
    order = ring_order(count)
    pairs = [(order[i], order[(i + step) % count]) for i in range(count)]
    return lax.ppermute(value, "tensor", pairs)


def ring_sources(own, count):
    place = jnp.where(own % 2 == 0, own // 2, count - 1 - own // 2)
    back = [(place - k) % count for k in range(count)]
    return [jnp.where(2 * p < count, 2 * p, 2 * (count - 1 - p) + 1) for p in back]


def ring_gather(value, last_step):
    count = lax.axis_size("tensor")
    ahead, back = value, value
    found = {0: value}
    for k in range(1, (count + 1) // 2):
        ahead = shift_in_ring(ahead, 1)
        back = shift_in_ring(back, -1)
        found[k], found[count - k] = ahead, back
    found[count // 2] = shift_in_ring(ahead if last_step > 0 else back, last_step)
    return [found[k] for k in range(count)]


def pair_owners(own, count):
    return [((own ^ (k % 2)) - 2 * (k // 2)) % count for k in range(count)]


def swap_pair(value):
    count = lax.axis_size("dp")
    return lax.ppermute(value, "dp", [(i, i ^ 1) for i in range(count)])


def shift_pairs(value):
    count = lax.axis_size("dp")
    return lax.ppermute(value, "dp", [(i, (i + 2) % count) for i in range(count)])


def pair_gather(value):
    count = lax.axis_size("dp")
    own = lax.axis_index("dp")
    found = []
    for k in range(count // 2):
        if k:
            value = shift_pairs(value)
        found.append(((own - 2 * k) % count, value))
        found.append((((own ^ 1) - 2 * k) % count, swap_pair(value)))
    return found


def finish_kernel(own_t, own_d, gain, early, *refs, counted, width):
    chunks, (hidden, normed) = refs[:-2], refs[-2:]
    features = normed.shape[1]
    squares = jnp.zeros((normed.shape[0], 128), jnp.float32)
    for k, chunk in enumerate(chunks):
        for i in range(0 if k in counted else chunk.shape[1] // 128):
            part = chunk[:, i * 128 : (i + 1) * 128].astype(jnp.float32)
            squares = squares + part * part
    scale = lax.rsqrt((jnp.sum(squares, axis=1, keepdims=True) + early[...]) / features + norm_eps)
    own_rows = pl.ds(pl.multiple_of(own_t[0] * hidden.shape[0], hidden.shape[0]), hidden.shape[0])
    per_chunk = chunks[0].shape[1] // width
    count_t = len(chunks) // 2
    sources = ring_sources(own_t[0], count_t)
    owners = pair_owners(own_d[0], 2 * per_chunk)
    for k, chunk in enumerate(chunks):
        for i in range(per_chunk):
            owner = owners[k % 2 * per_chunk + i]
            start = (owner * count_t + sources[k // 2]) * width
            columns = pl.ds(pl.multiple_of(start, 128), width)
            part = chunk[:, i * width : (i + 1) * width].astype(jnp.float32)
            normed[:, columns] = (part * scale * gain[:, columns].astype(jnp.float32)).astype(
                jnp.bfloat16
            )
            hidden[:, columns] = chunk[own_rows, i * width : (i + 1) * width]


def finish(chunks, squares, counted, own_count, norm_gain, width):
    rows = chunks[0].shape[0]
    features = norm_gain.shape[0]
    smem = pl.BlockSpec(memory_space=pltpu.SMEM)
    vmem = pl.BlockSpec(memory_space=pltpu.VMEM)
    return pl.pallas_call(
        lambda *refs: finish_kernel(*refs, counted=counted, width=width),
        out_shape=(
            jax.ShapeDtypeStruct((own_count, features), jnp.bfloat16),
            jax.ShapeDtypeStruct((rows, features), jnp.bfloat16),
        ),
        in_specs=[smem, smem] + [vmem] * (2 + len(chunks)),
        out_specs=(vmem, vmem),
        name="finish",
    )(
        lax.axis_index("tensor").reshape(1),
        lax.axis_index("dp").reshape(1),
        norm_gain.reshape(1, features),
        squares,
        *chunks,
    )


def exchanged_body(
    attn_input,
    residual,
    query_weight,
    query_bias,
    output_weight,
    cached_keys,
    cached_values,
    norm_gain,
):
    tok_count = attn_input.shape[0]
    ctx_len = cached_keys.shape[2]
    head_dim = cached_keys.shape[3]
    local_heads = query_weight.shape[1] // head_dim
    count_t = lax.axis_size("tensor")
    own_t = lax.axis_index("tensor")
    own_rows = query_weight.shape[0]
    shard_cols = output_weight.shape[1]
    width = shard_cols // count_t

    column_weight = lax.all_to_all(output_weight, "tensor", 1, 0, tiled=True)

    projected = query_bias.astype(jnp.float32)
    for owner, shard in pair_gather(query_weight):
        part = lax.dynamic_slice_in_dim(attn_input, owner * own_rows, own_rows, 1)
        projected = projected + jnp.dot(part, shard, preferred_element_type=jnp.float32)
    queries = rotate(
        projected.reshape(tok_count, local_heads, head_dim), float(ctx_len - tok_count)
    ).astype(jnp.bfloat16)
    mixed = attend(queries, cached_keys[0, 0], cached_values[0, 0]).reshape(
        tok_count, local_heads * head_dim
    )
    head_cols = mixed.shape[1]
    gathered = jnp.zeros((tok_count, count_t * head_cols), jnp.bfloat16)
    for source, got in zip(ring_sources(own_t, count_t), ring_gather(mixed, 1)):
        gathered = lax.dynamic_update_slice_in_dim(gathered, got, source * head_cols, 1)

    blocks = []
    for owner, shard in pair_gather(column_weight):
        summed = jnp.dot(gathered, shard, preferred_element_type=jnp.float32)
        start = owner * shard_cols + own_t * width
        resid = lax.dynamic_slice_in_dim(residual, start, width, 1).astype(jnp.float32)
        blocks.append((resid + summed).astype(jnp.bfloat16))
    count = len(blocks) // 2
    parts = [jnp.concatenate(blocks[i * count : (i + 1) * count], axis=1) for i in range(2)]
    near = ring_gather(parts[0], 1)
    early = (1, count_t - 1) if count_t > 2 else ()
    squares = sum(
        [jnp.sum(jnp.square(near[k].astype(jnp.float32)), axis=-1, keepdims=True) for k in early],
        jnp.zeros((tok_count, 1), jnp.float32),
    )
    far = ring_gather(parts[1], -1)
    chunks = [chunk for got in zip(near, far) for chunk in got]
    return finish(chunks, squares, [2 * k for k in early], tok_count // count_t, norm_gain, width)


def body(*arrays):
    output_weight = arrays[4]
    width = output_weight.shape[1] // lax.axis_size("tensor")
    if width % 128 or lax.axis_size("tensor") % 2 or lax.axis_size("dp") % 2:
        return gathered_body(*arrays)
    return exchanged_body(*arrays)


def solution(mesh):
    return jax.shard_map(
        body,
        mesh=mesh,
        in_specs=(
            P("dp", None),
            P("dp", None),
            P("dp", "tensor"),
            P("tensor"),
            P("tensor", "dp"),
            P("dp", "tensor", None, None),
            P("dp", "tensor", None, None),
            P(),
        ),
        out_specs=(P(("dp", "tensor"), None), P("dp", None)),
        check_vma=False,
    )
```
